16 devices in a mesh: data: 2 (over y, z), expert: 8 (over x, core).
Axes of the slice: x: 4, y: 2, z: 1, core: 2. Of those that a mesh axis runs over, the one named last changes fastest.
The devices are a block of a 4x4x8 slice.
Arguments:
- x: bfloat16 [4096, 2048], P(('data', 'expert')), parts along dimension 0
- idx: int32 [4096, 6], P(('data', 'expert')), parts along dimension 0
- g: float32 [4096, 6], P(('data', 'expert')), parts along dimension 0
- hot_tok: int32 [2048], P(('data', 'expert')), parts along dimension 0
- W1: bfloat16 [64, 2048, 1408], P('expert')
- W3: bfloat16 [64, 2048, 1408], P('expert')
- W2: bfloat16 [64, 1408, 2048], P('expert')
Outputs:
- output: bfloat16 [4096, 2048], P(('data', 'expert')), parts along dimension 0
There are 2 independent parts. The reference program is written for one: setup_inputs(seed, part) draws one part's arguments, and reference() takes and returns one part's arrays. A program takes and returns all parts, laid end to end along the dimension named above; an argument that names none is the same for every part.
All inputs are finite; a program needn't handle non-finite values.
Results may differ from the reference program's by a relative error of at most 0.001.
Values are sent between devices in bfloat16 or wider.
A program may use at most 768 MiB of HBM per device.

```python
import jax
import jax.numpy as jnp
from jax import lax

EXPERTS = 64
TOP = 6
D = 2048
FF = 1408
TOKENS = 256
HOT_DIV = 2
GROUP = 8

HOT_CAP = TOKENS // HOT_DIV
COLD_CAP = 2 * ((TOKENS * TOP - HOT_CAP + EXPERTS - 2) // (EXPERTS - 1))


def _weights(key, e, fan_in, fan_out):
    keys = jax.random.split(key, e)
    return lax.map(lambda k: (jax.random.normal(k, (fan_in, fan_out), jnp.float32) * fan_in ** -0.5).astype(jnp.bfloat16), keys)


def _chip_ids(key):
    k1, k2, k3 = jax.random.split(key, 3)
    t = jnp.arange(TOKENS)[:, None]
    j = jnp.arange(TOP)[None, :]
    hot = (t < HOT_CAP) & (j == 0)
    c = jnp.where(t < HOT_CAP, t * (TOP - 1) + j - 1, HOT_CAP * (TOP - 1) + (t - HOT_CAP) * TOP + j)
    seq = jnp.concatenate([jnp.arange(EXPERTS - 1), jnp.arange((EXPERTS - 1) // 2)])
    m = EXPERTS - 1 + (EXPERTS - 1) // 2
    off = jax.random.randint(k1, (), 0, m)
    perm = jax.random.permutation(k2, EXPERTS - 1)
    ids = jnp.flip(jnp.where(hot, 0, 1 + perm[seq[(c + off) % m]]), axis=1)
    shift = jax.random.randint(k3, (), 0, TOKENS)
    ids = jnp.roll(ids, shift, axis=0)
    hot_tok = jnp.sort((jnp.arange(HOT_CAP) + shift) % TOKENS)
    return ids.astype(jnp.int32), hot_tok.astype(jnp.int32)


def setup_inputs(seed: int = 0, part: int = 0) -> dict:
    kdata, kw = jax.random.split(jax.random.PRNGKey(seed))
    kx, kr, kg = jax.random.split(jax.random.fold_in(kdata, part), 3)
    k1, k3, k2 = jax.random.split(kw, 3)
    x = jax.random.normal(kx, (GROUP * TOKENS, D), jnp.float32).astype(jnp.bfloat16)
    ids, hot = jax.vmap(_chip_ids)(jax.random.split(jax.random.fold_in(kr, 7), GROUP))
    idx = ids.reshape(GROUP * TOKENS, TOP)
    u = jax.random.uniform(kg, (GROUP * TOKENS, TOP), jnp.float32)
    g = jnp.where(idx == 0, 0.6 + 0.4 * u, 0.2 + 0.5 * u)
    return {
        'x': x,
        'idx': idx,
        'g': g,
        'hot_tok': hot.reshape(GROUP * HOT_CAP),
        'W1': _weights(k1, EXPERTS, D, FF),
        'W3': _weights(k3, EXPERTS, D, FF),
        'W2': _weights(k2, EXPERTS, FF, D),
    }


def _expert(xr, w1, w3, w2):
    a = jnp.dot(xr, w1, preferred_element_type=jnp.float32)
    b = jnp.dot(xr, w3, preferred_element_type=jnp.float32)
    u = (jax.nn.silu(a) * b).astype(jnp.bfloat16)
    return jnp.dot(u, w2, preferred_element_type=jnp.float32).astype(jnp.bfloat16)


def reference(x, idx, g, hot_tok, W1, W3, W2):
    gate = jnp.where(idx == 0, g, 0.0).sum(axis=1)
    rows = (jnp.arange(GROUP)[:, None] * TOKENS + hot_tok.reshape(GROUP, HOT_CAP)).reshape(-1)
    hh = _expert(x[rows], W1[0], W3[0], W2[0]).astype(jnp.float32)
    y = jnp.zeros((GROUP * TOKENS, D), jnp.float32).at[rows].add(gate[rows][:, None] * hh)
    flat = idx.reshape(-1)
    order = jnp.argsort(flat, stable=True)
    counts = jnp.bincount(flat, length=EXPERTS)
    starts = jnp.cumsum(counts) - counts
    cap = GROUP * COLD_CAP
    order = jnp.concatenate([order, jnp.zeros((cap,), order.dtype)])
    gflat = g.reshape(-1)

    def step(y, ew):
        e, w1, w3, w2 = ew
        r = lax.dynamic_slice(order, (starts[e],), (cap,))
        valid = jnp.arange(cap) < counts[e]
        he = _expert(x[r // TOP], w1, w3, w2).astype(jnp.float32)
        return y.at[r // TOP].add(jnp.where(valid[:, None], gflat[r][:, None] * he, 0.0)), None

    y, _ = lax.scan(step, y, (jnp.arange(1, EXPERTS), W1[1:], W3[1:], W2[1:]))
    return y.astype(jnp.bfloat16)
```

```python
import functools

import jax
import jax.numpy as jnp
from jax import lax
from jax.experimental import pallas as pl
from jax.experimental.pallas import tpu as pltpu
from jax.sharding import PartitionSpec as P

MESH = pl.DeviceIdType.MESH
F32 = jnp.float32
BF16 = jnp.bfloat16
CHIPS = 4
PIECES = 4
FC = 256
DC = 256


def _dot(a, b):
    return jnp.dot(a, b, preferred_element_type=F32)


def _iota(shape, dim):
    return lax.broadcasted_iota(jnp.int32, shape, dim)


def _kernel(cap, hot, x_hbm, ig_hbm, w1_hbm, w3_hbm, w2_hbm, out_ref,
            xall, mall, pos, u, uhot, pown, psib, drecv, frecv, nrecv,
            loc_sem, xsend_s, xsend_r, xsend_l, xrecv, msend, mrecv,
            wsem, w2sem, dsend, drs, fsend, frs, nsend, nrs):
    me = lax.axis_index('expert')
    n = 2 * CHIPS
    c, k = me // 2, me % 2

    def dev(o, kk):
        return ((c + o) % CHIPS) * 2 + kk

    sib, right, left, far = dev(0, 1 - k), dev(1, k), dev(3, k), dev(2, k)
    t, d = x_hbm.shape
    el, _, ff = w1_hbm.shape
    nf = ff // FC
    tail = ff - nf * FC
    extra = hot - cap
    nq = d // DC
    half = DC // 2
    pt = t // PIECES

    def remote(src, dst, ss, rs, to):
        return pltpu.make_async_remote_copy(src_ref=src, dst_ref=dst, send_sem=ss, recv_sem=rs,
                                            device_id={'expert': to}, device_id_type=MESH)

    def phase_up(xg, xhot, wbuf, wtail, pmat, tri):
        def w_copies(e, f):
            if f < nf:
                return [pltpu.make_async_copy(w.at[e, :, pl.ds(f * FC, FC)], wbuf.at[f, :, pl.ds(s * FC, FC)], wsem.at[f, s])
                        for s, w in enumerate((w1_hbm, w3_hbm))]
            return [pltpu.make_async_copy(w.at[e, :, pl.ds(nf * FC, tail)], wtail.at[:, pl.ds(s * tail, tail)], wsem.at[nf, s])
                    for s, w in enumerate((w1_hbm, w3_hbm))]

        own = pltpu.make_async_copy(x_hbm, xall.at[me], loc_sem.at[0])
        own_m = pltpu.make_async_copy(ig_hbm, mall.at[me], loc_sem.at[1])
        own.start()
        own_m.start()
        barrier = pltpu.get_barrier_semaphore()
        for peer in (sib, right, left):
            pl.semaphore_signal(barrier, inc=1, device_id={'expert': peer}, device_id_type=MESH)
        pl.semaphore_wait(barrier, 3)
        own.wait()
        own_m.wait()

        def piece(b, p, ss, to):
            rows = pl.ds(p * pt, pt)
            return remote(xall.at[b, rows], xall.at[b, rows], ss, xrecv.at[b, p], to)

        def meta(b, ss, to):
            return remote(mall.at[b], mall.at[b], ss, mrecv.at[b], to)

        sends = []

        def go(copy):
            copy.start()
            sends.append(copy)

        go(meta(me, msend.at[0], sib))
        go(meta(me, msend.at[1], right))
        go(meta(me, msend.at[2], left))
        for p in range(PIECES):
            q = (p + PIECES // 2) % PIECES
            go(piece(me, p, xsend_r.at[p], right))
            go(piece(me, q, xsend_l.at[q], left))
        for p in range(PIECES):
            go(piece(me, p, xsend_s.at[0, p], sib))
        for e_f in range(nf + 1):
            for cp in w_copies(0, e_f):
                cp.start()

        def got(b, p):
            piece(b, p, xsend_s.at[0, p], sib).wait_recv()

        def got_meta(b):
            meta(b, msend.at[0], sib).wait_recv()

        tri[...] = (_iota((t, t), 0) < _iota((t, t), 1)).astype(BF16)

        def gather(b):
            ids = mall[b, 0:8]
            gts = mall[b, 8:16]
            for e in range(el):
                eq = ids == (me * el + e).astype(F32)
                pos[0, b, e:e + 1, :] = jnp.sum(eq.astype(F32), axis=0, keepdims=True)
                pos[1, b, e:e + 1, :] = jnp.sum(jnp.where(eq, gts, 0.0), axis=0, keepdims=True)
            m = pos[0, b]
            before = _dot(m.astype(BF16), tri[...])
            rank = jnp.where(m > 0.0, before, -1.0)
            pos[0, b] = rank
            row = _iota((cap, t), 0).astype(F32)
            for e in range(el):
                pmat[e] = (rank[e:e + 1, :] == row).astype(BF16)
            sel = pmat[...].reshape(el * cap, t)

            def cols(j, _):
                w = pl.ds(pl.multiple_of(j * 512, 512), 512)
                r = _dot(sel, xall[b, :, w]).astype(BF16).reshape(el, cap, 512)
                for e in range(el):
                    xg[e, b, :, w] = r[e]
                return 0

            lax.fori_loop(0, d // 512, cols, 0)

            @pl.when(me == 0)
            def _():
                hrow = _iota((extra, t), 0).astype(F32) + float(cap)
                hsel = (rank[0:1, :] == hrow).astype(BF16)

                def hcols(j, _):
                    w = pl.ds(pl.multiple_of(j * 512, 512), 512)
                    xhot[b, :, w] = _dot(hsel, xall[b, :, w]).astype(BF16)
                    return 0

                lax.fori_loop(0, d // 512, hcols, 0)

        gather_later = []
        hp = PIECES // 2
        gather(me)
        got_meta(left)
        go(meta(left, msend.at[3], right))
        go(meta(left, msend.at[4], sib))
        got_meta(right)
        go(meta(right, msend.at[5], sib))
        for p in range(hp):
            got(left, p)
            go(piece(left, p, xsend_r.at[PIECES + p], right))
            go(piece(left, p, xsend_s.at[1, p], sib))
            got(right, hp + p)
            go(piece(right, hp + p, xsend_l.at[PIECES + p], left))
            go(piece(right, hp + p, xsend_s.at[2, hp + p], sib))
        for p in range(hp):
            got(left, hp + p)
            go(piece(left, hp + p, xsend_s.at[1, hp + p], sib))
            got(right, p)
            go(piece(right, p, xsend_s.at[2, p], sib))

        def rest(b):
            got_meta(b)
            for p in range(PIECES):
                got(b, p)
            gather(b)

        gather(left)
        gather(right)
        rest(sib)
        got_meta(far)
        go(meta(far, msend.at[6], sib))
        for p in range(hp):
            got(far, p)
            go(piece(far, p, xsend_s.at[3, p], sib))
            got(far, hp + p)
            go(piece(far, hp + p, xsend_s.at[3, hp + p], sib))
        rest(dev(3, 1 - k))
        rest(dev(1, 1 - k))
        gather(far)
        rest(dev(2, 1 - k))

        def up(e, _):
            lhs = xg[e].reshape(n * cap, d)

            def act(rows, w, width):
                ab = _dot(rows, w)
                a, b = ab[:, :width], ab[:, width:]
                return (a * jax.nn.sigmoid(a) * b).astype(BF16)

            for f in range(nf + 1):
                for cp in w_copies(e, f):
                    cp.wait()
                w_ref, width = (wbuf.at[f], FC) if f < nf else (wtail, tail)
                w_cols = pl.ds(f * FC, width)
                u[e, :, w_cols] = act(lhs, w_ref[...], width)

                @pl.when(jnp.logical_and(me == 0, e == 0))
                def _():
                    hr = n * extra // 2
                    for s in range(2):
                        rows = xhot[s * (n // 2):(s + 1) * (n // 2)].reshape(hr, d)
                        uhot[s * hr:(s + 1) * hr, w_cols] = act(rows, w_ref[...], width)

                @pl.when(e + 1 < el)
                def _():
                    for cp in w_copies(jnp.minimum(e + 1, el - 1), f):
                        cp.start()
            return 0

        lax.fori_loop(0, el, up, 0)
        for copy in sends:
            copy.wait_send()

    pl.run_scoped(phase_up,
                  pltpu.VMEM((el, n, cap, d), BF16), pltpu.VMEM((n, extra, d), BF16),
                  pltpu.VMEM((nf, d, 2 * FC), BF16), pltpu.VMEM((d, 2 * tail), BF16),
                  pltpu.VMEM((el, cap, t), BF16), pltpu.VMEM((t, t), BF16))

    def phase_down(w2buf, s_all, s_hot, hbuf, hhot, cat):
        def w2_copy(q, e):
            cols = pl.ds(pl.multiple_of(q * DC, DC), DC)
            return pltpu.make_async_copy(w2_hbm.at[e, :, cols], w2buf.at[e], w2sem.at[e])

        for e in range(el):
            w2_copy(0, e).start()

        for b in range(n):
            cat[b * el:(b + 1) * el, :] = pos[0, b]
            cat[(n + b) * el:(n + b + 1) * el, :] = pos[1, b]
        cols = jnp.transpose(cat[...])
        g1 = cols.astype(BF16)
        r1 = cols - g1.astype(F32)
        g2 = r1.astype(BF16)
        g3 = (r1 - g2.astype(F32)).astype(BF16)
        lane = _iota((1, el * cap), 1)
        slot_e = jnp.zeros((1, el * cap), jnp.int32)
        for e in range(1, el):
            slot_e = slot_e + (lane >= e * cap).astype(jnp.int32)
        want = (lane - cap * slot_e).astype(F32)

        def build(b, _):
            rr = _iota((2 * n * el, el * cap), 0)
            lo = (rr - b * el) * cap
            ll = _iota((2 * n * el, el * cap), 1)
            pick = jnp.logical_and(ll >= lo, ll < lo + cap).astype(BF16)
            lo2 = lo - n * el * cap
            pick2 = jnp.logical_and(ll >= lo2, ll < lo2 + cap).astype(BF16)
            hit = _dot(g1, pick) == want
            for s, gs in enumerate((g1, g2, g3)):
                s_all[b, s] = jnp.where(hit, _dot(gs, pick2), 0.0).astype(BF16)

            @pl.when(me == 0)
            def _():
                rh = _iota((2 * n * el, extra), 0)
                hpick = (rh == b * el).astype(BF16)
                hpick2 = (rh == (n + b) * el).astype(BF16)
                hhit = _dot(g1, hpick) == (_iota((t, extra), 1) + cap).astype(F32)
                for s, gs in enumerate((g1, g2, g3)):
                    s_hot[b, s] = jnp.where(hhit, _dot(gs, hpick2), 0.0).astype(BF16)

            return 0

        lax.fori_loop(0, n, build, 0)

        def d_copy(q):
            return remote(psib.at[q % 2], drecv.at[q % 2], dsend.at[q % 2], drs.at[q % 2], sib)

        def f_copies(q):
            return [remote(pown.at[q % 4, 2, s], frecv.at[q % 2, s], fsend.at[q % 4, s], frs.at[q % 2, s], to)
                    for s, to in enumerate((right, left))]

        def n_copies(q):
            return [remote(pown.at[q % 4, o], nrecv.at[q % 2, s], nsend.at[q % 4, s], nrs.at[q % 2, s], to)
                    for s, (o, to) in enumerate(((1, right), (3, left)))]

        def step(i, _):
            @pl.when(i >= 3)
            def _():
                q = i - 3
                for cp in n_copies(q):
                    cp.wait_recv()
                for s in range(2):
                    y = pown[q % 4, 0, s] + nrecv[q % 2, 0, s] + nrecv[q % 2, 1, s]
                    out_ref[:, pl.ds(pl.multiple_of(q * DC + s * half, half), half)] = y.astype(BF16)

            @pl.when(jnp.logical_and(i >= 1, i <= nq))
            def _():
                q = i - 1
                d_copy(q).wait_recv()
                for o in (2, 1, 3, 0):
                    pown[q % 4, o] = pown[q % 4, o] + drecv[q % 2, o]
                for cp in f_copies(q):
                    cp.start()

            @pl.when(jnp.logical_and(i >= 2, i <= nq + 1))
            def _():
                q = i - 2
                for cp in f_copies(q):
                    cp.wait_recv()
                pown[q % 4, 1, 0] = pown[q % 4, 1, 0] + frecv[q % 2, 0]
                pown[q % 4, 3, 1] = pown[q % 4, 3, 1] + frecv[q % 2, 1]
                for cp in n_copies(q):
                    cp.start()

            @pl.when(i < nq)
            def _():
                q = i

                def down(e, _):
                    w2_copy(q, e).wait()
                    h = _dot(u[e], w2buf[e]).astype(BF16).reshape(n, cap, DC)
                    for b in range(n):
                        hbuf[b, e] = h[b]

                    @pl.when(jnp.logical_and(me == 0, e == 0))
                    def _():
                        hhot[...] = _dot(uhot[...], w2buf[e]).astype(BF16).reshape(n, extra, DC)

                    @pl.when(q + 1 < nq)
                    def _():
                        w2_copy(jnp.minimum(q + 1, nq - 1), e).start()

                    return 0

                lax.fori_loop(0, el, down, 0)

                @pl.when(i >= 4)
                def _():
                    for cp in f_copies(q - 4) + n_copies(q - 4):
                        cp.wait_send()

                @pl.when(i >= 2)
                def _():
                    d_copy(q - 2).wait_send()

                def scatter(o, _):
                    for kk, dst in ((1 - k, psib.at[q % 2, o]), (k, pown.at[q % 4, o])):
                        b = dev(o, kk)
                        r = _dot(s_all[b].reshape(3 * t, el * cap), hbuf[b].reshape(el * cap, DC))
                        r = r[:t] + r[t:2 * t] + r[2 * t:]
                        dst[0] = r[:, :half]
                        dst[1] = r[:, half:]

                        @pl.when(me == 0)
                        def _():
                            z = _dot(s_hot[b].reshape(3 * t, extra), hhot[b])
                            z = z[:t] + z[t:2 * t] + z[2 * t:]
                            dst[0] = dst[0] + z[:, :half]
                            dst[1] = dst[1] + z[:, half:]

                    return 0

                lax.fori_loop(0, CHIPS, scatter, 0)
                d_copy(q).start()

            return 0

        lax.fori_loop(0, nq + 3, step, 0)
        for q in range(nq - 4, nq):
            for cp in f_copies(q) + n_copies(q):
                cp.wait_send()
        for q in range(nq - 2, nq):
            d_copy(q).wait_send()

    pl.run_scoped(phase_down,
                  pltpu.VMEM((el, ff, DC), BF16), pltpu.VMEM((n, 3, t, el * cap), BF16),
                  pltpu.VMEM((n, 3, t, extra), BF16), pltpu.VMEM((n, el, cap, DC), BF16),
                  pltpu.VMEM((n, extra, DC), BF16), pltpu.VMEM((2 * n * el, t), F32))


def solution(mesh):
    n = mesh.shape['expert']
    assert n == 2 * CHIPS

    def local(x, idx, g, hot_tok, w1, w3, w2):
        t, d = x.shape
        k = idx.shape[1]
        el, _, ff = w1.shape
        e = el * n
        hot = hot_tok.shape[0]
        most = 2 * ((t * k - hot + e - 2) // (e - 1))
        cap = -(-most // 16) * 16
        extra = hot - cap
        half = DC // 2
        pad = jnp.full((8 - k, t), -1.0, F32)
        ig = jnp.concatenate([idx.T.astype(F32), pad, g.T, pad])
        dma, any_ = pltpu.SemaphoreType.DMA, pl.BlockSpec(memory_space=pl.ANY)
        return pl.pallas_call(
            functools.partial(_kernel, cap, hot),
            out_shape=jax.ShapeDtypeStruct((t, d), BF16),
            in_specs=[any_] * 5,
            out_specs=pl.BlockSpec(memory_space=pltpu.VMEM),
            scratch_shapes=[
                pltpu.VMEM((n, t, d), BF16), pltpu.VMEM((n, 16, t), F32), pltpu.VMEM((2, n, el, t), F32),
                pltpu.VMEM((el, n * cap, ff), BF16), pltpu.VMEM((n * extra, ff), BF16),
                pltpu.VMEM((4, CHIPS, 2, t, half), F32), pltpu.VMEM((2, CHIPS, 2, t, half), F32),
                pltpu.VMEM((2, CHIPS, 2, t, half), F32), pltpu.VMEM((2, 2, t, half), F32),
                pltpu.VMEM((2, 2, 2, t, half), F32),
                dma((2,)), dma((4, PIECES)), dma((2 * PIECES,)), dma((2 * PIECES,)), dma((n, PIECES)), dma((7,)), dma((n,)),
                dma((ff // FC + 1, 2)), dma((el,)), dma((2,)), dma((2,)), dma((4, 2)), dma((2, 2)), dma((4, 2)), dma((2, 2)),
            ],
            compiler_params=pltpu.CompilerParams(collective_id=0, has_side_effects=True, vmem_limit_bytes=67043328),
        )(x, ig, w1, w3, w2)

    rows = P(('data', 'expert'))
    wspec = P('expert')
    return jax.shard_map(local, mesh=mesh, in_specs=(rows, rows, rows, rows, wspec, wspec, wspec), out_specs=rows, check_vma=False)
```

```python
import functools

import jax
import jax.numpy as jnp
from jax import lax
from jax.experimental import pallas as pl
from jax.experimental.pallas import tpu as pltpu
from jax.sharding import PartitionSpec as P

MESH = pl.DeviceIdType.MESH
F32 = jnp.float32
BF16 = jnp.bfloat16
CHIPS = 4
PIECES = 4
FC = 256
DC = 256


def _dot(a, b):
    return jnp.dot(a, b, preferred_element_type=F32)


def _iota(shape, dim):
    return lax.broadcasted_iota(jnp.int32, shape, dim)


def _kernel(cap, hot, x_hbm, ig_hbm, w1_hbm, w3_hbm, w2_hbm, out_ref,
            xall, mall, pos, xg, xhot, u, uhot, wbuf, wtail, w2buf, s_all, s_hot, hbuf, hhot,
            pown, psib, drecv, frecv, nrecv, cat, pmat, tri,
            loc_sem, xsend_s, xsend_r, xsend_l, xrecv, msend, mrecv,
            wsem, w2sem, dsend, drs, fsend, frs, nsend, nrs, credit):
    me = lax.axis_index('expert')
    c, k = me // 2, me % 2

    def dev(o, kk):
        return ((c + o) % CHIPS) * 2 + kk

    sib, right, left, far = dev(0, 1 - k), dev(1, k), dev(3, k), dev(2, k)
    t, d = x_hbm.shape
    el, _, ff = w1_hbm.shape
    nf = ff // FC
    tail = ff - nf * FC
    extra = hot - cap
    nq = d // DC
    half = DC // 2
    pt = t // PIECES
    hp = PIECES // 2
    rows = CHIPS * cap

    def remote(src, dst, ss, rs, to):
        return pltpu.make_async_remote_copy(src_ref=src, dst_ref=dst, send_sem=ss, recv_sem=rs,
                                            device_id={'expert': to}, device_id_type=MESH)

    def w_copies(e, f):
        if f < nf:
            return [pltpu.make_async_copy(w.at[e, :, pl.ds(f * FC, FC)], wbuf.at[f, :, pl.ds(s * FC, FC)], wsem.at[f, s])
                    for s, w in enumerate((w1_hbm, w3_hbm))]
        return [pltpu.make_async_copy(w.at[e, :, pl.ds(nf * FC, tail)], wtail.at[:, pl.ds(s * tail, tail)], wsem.at[nf, s])
                for s, w in enumerate((w1_hbm, w3_hbm))]

    def w2_copy(q, e):
        cols = pl.ds(pl.multiple_of(q * DC, DC), DC)
        return pltpu.make_async_copy(w2_hbm.at[e, :, cols], w2buf.at[e], w2sem.at[e])

    def piece(b, p, ss, to):
        r = pl.ds(p * pt, pt)
        return remote(xall.at[b, r], xall.at[b, r], ss, xrecv.at[b, p], to)

    def meta(b, ss, to):
        return remote(mall.at[b], mall.at[b], ss, mrecv.at[b], to)

    def got(b, p):
        piece(b, p, xsend_s.at[0, p], sib).wait_recv()

    def got_meta(b):
        meta(b, msend.at[0], sib).wait_recv()

    def to_sib(o, p):
        return piece(dev(o, k), p, xsend_s.at[o, p], sib)

    def own_right(p):
        return piece(me, p, xsend_r.at[p], right)

    def own_left(p):
        return piece(me, p, xsend_l.at[p], left)

    def relay_right(p):
        return piece(left, p, xsend_r.at[PIECES + p], right)

    def relay_left(p):
        return piece(right, hp + p, xsend_l.at[PIECES + p], left)

    def token_sends():
        out = [to_sib(o, p) for o in range(CHIPS) for p in range(PIECES)]
        out += [own_right(p) for p in range(PIECES)] + [own_left(p) for p in range(PIECES)]
        return out + [relay_right(p) for p in range(hp)] + [relay_left(p) for p in range(hp)]

    def send_own():
        for p in range(PIECES):
            own_right(p).start()
            own_left((p + hp) % PIECES).start()
        for p in range(PIECES):
            to_sib(0, p).start()

    def relay(p):
        got(left, p)
        relay_right(p).start()
        got(right, hp + p)
        relay_left(p).start()

    def sib_near(first):
        for p in range(hp):
            q = p if first else hp + p
            to_sib(3, q).start()
            to_sib(1, hp + p if first else p).start()

    def rest_near():
        for p in range(hp):
            got(left, hp + p)
            got(right, p)

    def far_in():
        for p in range(hp):
            got(far, p)
            to_sib(2, p).start()
            got(far, hp + p)
            to_sib(2, hp + p).start()

    def wait_block(b):
        for p in range(PIECES):
            got(b, p)

    def gather(beta, o):
        b = dev(o, beta)
        ids = mall[b, 0:8]
        gts = mall[b, 8:16]
        for e in range(el):
            eq = ids == (me * el + e).astype(F32)
            pos[0, o, e:e + 1, :] = jnp.sum(eq.astype(F32), axis=0, keepdims=True)
            pos[1, o, e:e + 1, :] = jnp.sum(jnp.where(eq, gts, 0.0), axis=0, keepdims=True)
        m = pos[0, o]
        before = _dot(m.astype(BF16), tri[...])
        rank = jnp.where(m > 0.0, before, -1.0)
        pos[0, o] = rank
        row = _iota((cap, t), 0).astype(F32)
        for e in range(el):
            pmat[e] = (rank[e:e + 1, :] == row).astype(BF16)
        sel = pmat[...].reshape(el * cap, t)

        def cols(j, _):
            w = pl.ds(pl.multiple_of(j * 512, 512), 512)
            r = _dot(sel, xall[b, :, w]).astype(BF16).reshape(el, cap, 512)
            for e in range(el):
                xg[e, o, :, w] = r[e]
            return 0

        lax.fori_loop(0, d // 512, cols, 0)

        @pl.when(me == 0)
        def _():
            hrow = _iota((extra, t), 0).astype(F32) + float(cap)
            hsel = (rank[0:1, :] == hrow).astype(BF16)

            def hcols(j, _):
                w = pl.ds(pl.multiple_of(j * 512, 512), 512)
                xhot[o, :, w] = _dot(hsel, xall[b, :, w]).astype(BF16)
                return 0

            lax.fori_loop(0, d // 512, hcols, 0)

    def up(beta, hook):
        def body(i, _):
            e = i if beta == 0 else el - 1 - i
            after = jnp.minimum(e + 1, el - 1) if beta == 0 else jnp.maximum(e - 1, 0)
            hook(i)
            lhs = xg[e].reshape(rows, d)

            def act(r, w, width):
                ab = _dot(r, w)
                a, b = ab[:, :width], ab[:, width:]
                return (a * jax.nn.sigmoid(a) * b).astype(BF16)

            for f in range(nf + 1):
                if beta == 0:
                    for cp in w_copies(e, f):
                        cp.wait()
                else:
                    @pl.when(i > 0)
                    def _():
                        for cp in w_copies(e, f):
                            cp.wait()
                w_ref, width = (wbuf.at[f], FC) if f < nf else (wtail, tail)
                w_cols = pl.ds(f * FC, width)
                u[e, :, w_cols] = act(lhs, w_ref[...], width)

                @pl.when(jnp.logical_and(me == 0, e == 0))
                def _():
                    uhot[:, w_cols] = act(xhot[...].reshape(CHIPS * extra, d), w_ref[...], width)

                @pl.when(i + 1 < el)
                def _():
                    for cp in w_copies(after, f):
                        cp.start()
            return 0

        lax.fori_loop(0, el, body, 0)

    def d_copy(q):
        return remote(psib.at[q % 2], drecv.at[q % 2], dsend.at[q % 2], drs.at[q % 2], sib)

    def f_copies(q):
        return [remote(pown.at[q, 2, s], frecv.at[q, s], fsend.at[q, s], frs.at[q, s], to)
                for s, to in enumerate((right, left))]

    def n_copies(q):
        return [remote(pown.at[q, o], nrecv.at[q, s], nsend.at[q, s], nrs.at[q, s], to)
                for s, (o, to) in enumerate(((1, right), (3, left)))]

    def pair_add(q):
        d_copy(q).wait_recv()
        for o in (2, 1, 3, 0):
            pown[q, o] = psib[q % 2, o] + drecv[q % 2, o]
        for cp in f_copies(q):
            cp.start()

        @pl.when(q < nq - 2)
        def _():
            pl.semaphore_signal(credit, inc=1, device_id={'expert': sib}, device_id_type=MESH)

    def relay_add(q):
        for cp in f_copies(q):
            cp.wait_recv()
        pown[q, 1, 0] = pown[q, 1, 0] + frecv[q, 0]
        pown[q, 3, 1] = pown[q, 3, 1] + frecv[q, 1]
        for cp in n_copies(q):
            cp.start()

    def finish(q, _):
        for cp in n_copies(q):
            cp.wait_recv()
        for s in range(2):
            y = pown[q, 0, s] + nrecv[q, 0, s] + nrecv[q, 1, s]
            out_ref[:, pl.ds(pl.multiple_of(q * DC + s * half, half), half)] = y.astype(BF16)
        return 0

    def build_scatter():
        cat[...] = jnp.zeros_like(cat)
        for o in range(CHIPS):
            cat[o * el:(o + 1) * el, :] = pos[0, o]
            cat[(CHIPS + o) * el:(CHIPS + o + 1) * el, :] = pos[1, o]
        cols = jnp.transpose(cat[...])
        g1 = cols.astype(BF16)
        r1 = cols - g1.astype(F32)
        g2 = r1.astype(BF16)
        g3 = (r1 - g2.astype(F32)).astype(BF16)
        lane = _iota((1, el * cap), 1)
        slot_e = jnp.zeros((1, el * cap), jnp.int32)
        for e in range(1, el):
            slot_e = slot_e + (lane >= e * cap).astype(jnp.int32)
        want = (lane - cap * slot_e).astype(F32)
        depth = cat.shape[0]

        def build(o, _):
            rr = _iota((depth, el * cap), 0)
            ll = _iota((depth, el * cap), 1)
            lo = (rr - o * el) * cap
            pick = jnp.logical_and(ll >= lo, ll < lo + cap).astype(BF16)
            lo2 = lo - CHIPS * el * cap
            pick2 = jnp.logical_and(ll >= lo2, ll < lo2 + cap).astype(BF16)
            hit = _dot(g1, pick) == want
            for s, gs in enumerate((g1, g2, g3)):
                s_all[o, s] = jnp.where(hit, _dot(gs, pick2), 0.0).astype(BF16)

            @pl.when(me == 0)
            def _():
                rh = _iota((depth, extra), 0)
                hpick = (rh == o * el).astype(BF16)
                hpick2 = (rh == (CHIPS + o) * el).astype(BF16)
                hhit = _dot(g1, hpick) == (_iota((t, extra), 1) + cap).astype(F32)
                for s, gs in enumerate((g1, g2, g3)):
                    s_hot[o, s] = jnp.where(hhit, _dot(gs, hpick2), 0.0).astype(BF16)

            return 0

        lax.fori_loop(0, CHIPS, build, 0)

    def chunk(beta, q):
        def down(e, _):
            w2_copy(q, e).wait()
            h = _dot(u[e], w2buf[e]).astype(BF16).reshape(CHIPS, cap, DC)
            for o in range(CHIPS):
                hbuf[o, e] = h[o]

            @pl.when(jnp.logical_and(me == 0, e == 0))
            def _():
                hhot[...] = _dot(uhot[...], w2buf[e]).astype(BF16).reshape(CHIPS, extra, DC)

            if beta == 0:
                w2_copy((q + 1) % nq, e).start()
            else:
                @pl.when(q + 1 < nq)
                def _():
                    w2_copy(jnp.minimum(q + 1, nq - 1), e).start()

            return 0

        lax.fori_loop(0, el, down, 0)

        @pl.when(jnp.logical_and(k != beta, q >= 2))
        def _():
            d_copy(q - 2).wait_send()

        def scatter(o, _):
            r = _dot(s_all[o].reshape(3 * t, el * cap), hbuf[o].reshape(el * cap, DC))
            r = r[:t] + r[t:2 * t] + r[2 * t:]
            psib[q % 2, o, 0] = r[:, :half]
            psib[q % 2, o, 1] = r[:, half:]

            @pl.when(me == 0)
            def _():
                z = _dot(s_hot[o].reshape(3 * t, extra), hhot[o])
                z = z[:t] + z[t:2 * t] + z[2 * t:]
                psib[q % 2, o, 0] = psib[q % 2, o, 0] + z[:, :half]
                psib[q % 2, o, 1] = psib[q % 2, o, 1] + z[:, half:]

            return 0

        lax.fori_loop(0, CHIPS, scatter, 0)

        @pl.when(k != beta)
        def _():
            @pl.when(q >= 2)
            def _():
                pl.semaphore_wait(credit, 1)
            d_copy(q).start()

    def down_phase(beta):
        build_scatter()
        last = nq + 1 if beta == 0 else nq + 3

        def step(i, _):
            @pl.when(jnp.logical_and(k == beta, jnp.logical_and(i >= 1, i <= nq)))
            def _():
                pair_add(i - 1)

            if beta == 0:
                for at, q in ((3, 0), (5, 1), (7, 2)):
                    @pl.when(jnp.logical_and(k == beta, i == at))
                    def _():
                        relay_add(q)
            else:
                @pl.when(jnp.logical_and(k == beta, i >= 3))
                def _():
                    relay_add(i - 3)

            @pl.when(i < nq)
            def _():
                chunk(beta, i)

            return 0

        lax.fori_loop(0, last, step, 0)

        @pl.when(k != beta)
        def _():
            for q in range(nq - 2, nq):
                d_copy(q).wait_send()

    own = pltpu.make_async_copy(x_hbm, xall.at[me], loc_sem.at[0])
    own_m = pltpu.make_async_copy(ig_hbm, mall.at[me], loc_sem.at[1])
    own.start()
    own_m.start()
    barrier = pltpu.get_barrier_semaphore()
    for peer in (sib, right, left):
        pl.semaphore_signal(barrier, inc=1, device_id={'expert': peer}, device_id_type=MESH)
    pl.semaphore_wait(barrier, 3)
    own.wait()
    own_m.wait()
    metas = [meta(me, msend.at[0], sib), meta(me, msend.at[1], right), meta(me, msend.at[2], left)]
    for cp in metas:
        cp.start()

    @pl.when(k == 0)
    def _():
        send_own()

    for f in range(nf + 1):
        for cp in w_copies(0, f):
            cp.start()
    for e in range(el):
        w2_copy(0, e).start()
    tri[...] = (_iota((t, t), 0) < _iota((t, t), 1)).astype(BF16)

    got_meta(left)
    metas += [meta(left, msend.at[3], right), meta(left, msend.at[4], sib)]
    metas[3].start()
    metas[4].start()
    got_meta(right)
    metas += [meta(right, msend.at[5], sib)]
    metas[5].start()
    got_meta(far)
    metas += [meta(far, msend.at[6], sib)]
    metas[6].start()
    for o in range(CHIPS):
        got_meta(dev(o, 1 - k))

    @pl.when(k == 1)
    def _():
        wait_block(dev(0, 0))

    gather(0, 0)

    @pl.when(k == 0)
    def _():
        for p in range(hp):
            relay(p)
        sib_near(True)
        rest_near()
        sib_near(False)

    @pl.when(k == 1)
    def _():
        wait_block(dev(3, 0))
        wait_block(dev(1, 0))

    gather(0, 3)
    gather(0, 1)

    @pl.when(k == 0)
    def _():
        far_in()

    @pl.when(k == 1)
    def _():
        wait_block(dev(2, 0))
        send_own()

    gather(0, 2)

    def hook_first(i):
        @pl.when(k == 1)
        def _():
            for at, p in ((1, 0), (2, 1)):
                @pl.when(i == at)
                def _():
                    relay(p)

            @pl.when(i == 4)
            def _():
                rest_near()
                sib_near(True)
                sib_near(False)

            @pl.when(i == 6)
            def _():
                far_in()

    up(0, hook_first)
    down_phase(0)

    @pl.when(k == 0)
    def _():
        for o in range(CHIPS):
            wait_block(dev(o, 1))

    for o in range(CHIPS):
        gather(1, o)

    def hook_second(i):
        @pl.when(jnp.logical_and(k == 0, i < nq - 3))
        def _():
            relay_add(3 + i)

    up(1, hook_second)
    down_phase(1)
    lax.fori_loop(0, nq, finish, 0)

    for cp in metas:
        cp.wait_send()
    for cp in token_sends():
        cp.wait_send()
    for q in range(nq):
        for cp in f_copies(q) + n_copies(q):
            cp.wait_send()


def solution(mesh):
    n = mesh.shape['expert']
    assert n == 2 * CHIPS

    def local(x, idx, g, hot_tok, w1, w3, w2):
        t, d = x.shape
        k = idx.shape[1]
        el, _, ff = w1.shape
        e = el * n
        hot = hot_tok.shape[0]
        most = 2 * ((t * k - hot + e - 2) // (e - 1))
        cap = -(-most // 16) * 16
        extra = hot - cap
        half = DC // 2
        nf, nq = ff // FC, d // DC
        tail = ff - nf * FC
        pad = jnp.full((8 - k, t), -1.0, F32)
        ig = jnp.concatenate([idx.T.astype(F32), pad, g.T, pad])
        dma, any_ = pltpu.SemaphoreType.DMA, pl.BlockSpec(memory_space=pl.ANY)
        vm = pltpu.VMEM
        return pl.pallas_call(
            functools.partial(_kernel, cap, hot),
            out_shape=jax.ShapeDtypeStruct((t, d), BF16),
            in_specs=[any_] * 5,
            out_specs=pl.BlockSpec(memory_space=pltpu.VMEM),
            scratch_shapes=[
                vm((n, t, d), BF16), vm((n, 16, t), F32), vm((2, CHIPS, el, t), F32),
                vm((el, CHIPS, cap, d), BF16), vm((CHIPS, extra, d), BF16),
                vm((el, CHIPS * cap, ff), BF16), vm((CHIPS * extra, ff), BF16),
                vm((nf, d, 2 * FC), BF16), vm((d, 2 * tail), BF16), vm((el, ff, DC), BF16),
                vm((CHIPS, 3, t, el * cap), BF16), vm((CHIPS, 3, t, extra), BF16),
                vm((CHIPS, el, cap, DC), BF16), vm((CHIPS, extra, DC), BF16),
                vm((nq, CHIPS, 2, t, half), F32), vm((2, CHIPS, 2, t, half), F32), vm((2, CHIPS, 2, t, half), F32),
                vm((nq, 2, t, half), F32), vm((nq, 2, 2, t, half), F32),
                vm((-(-2 * CHIPS * el // 128) * 128, t), F32), vm((el, cap, t), BF16), vm((t, t), BF16),
                dma((2,)), dma((CHIPS, PIECES)), dma((2 * PIECES,)), dma((2 * PIECES,)), dma((n, PIECES)), dma((7,)), dma((n,)),
                dma((nf + 1, 2)), dma((el,)), dma((2,)), dma((2,)), dma((nq, 2)), dma((nq, 2)), dma((nq, 2)), dma((nq, 2)),
                pltpu.SemaphoreType.REGULAR,
            ],
            compiler_params=pltpu.CompilerParams(collective_id=0, has_side_effects=True, vmem_limit_bytes=67043328),
        )(x, ig, w1, w3, w2)

    rows = P(('data', 'expert'))
    wspec = P('expert')
    return jax.shard_map(local, mesh=mesh, in_specs=(rows, rows, rows, rows, wspec, wspec, wspec), out_specs=rows, check_vma=False)
```

```python
import functools

import jax
import jax.numpy as jnp
from jax import lax
from jax.experimental import pallas as pl
from jax.experimental.pallas import tpu as pltpu
from jax.sharding import PartitionSpec as P

MESH = pl.DeviceIdType.MESH
F32 = jnp.float32
BF16 = jnp.bfloat16
CHIPS = 4
PIECES = 4
FC = 256
DC = 256


def _dot(a, b):
    return jnp.dot(a, b, preferred_element_type=F32)


def _iota(shape, dim):
    return lax.broadcasted_iota(jnp.int32, shape, dim)


def _kernel(cap, hot, x_hbm, idx_hbm, g_hbm, w1_hbm, w3_hbm, w2_hbm, out_ref,
            xall, mall, pos, xg, xhot, u, uhot, wbuf, wtail, w2buf, s_all, hbuf,
            pown, psib, drecv, frecv, nrecv, cat, pmat, phot, tri, idx_v, g_v, turn,
            loc_sem, xsend_s, xsend_r, xsend_l, xrecv, msend, mrecv,
            wsem, w2sem, dsend, drs, fsend, frs, nsend, nrs, credit):
    me = lax.axis_index('expert')
    c, k = me // 2, me % 2

    def dev(o, kk):
        return ((c + o) % CHIPS) * 2 + kk

    sib, right, left, far = dev(0, 1 - k), dev(1, k), dev(3, k), dev(2, k)
    t, d = x_hbm.shape
    top = idx_hbm.shape[1]
    el, _, ff = w1_hbm.shape
    nf = ff // FC
    tail = ff - nf * FC
    extra = hot - cap
    nq = d // DC
    half = DC // 2
    pt = t // PIECES
    hp = PIECES // 2
    rows = CHIPS * cap
    wide = el * cap + extra

    def remote(src, dst, ss, rs, to):
        return pltpu.make_async_remote_copy(src_ref=src, dst_ref=dst, send_sem=ss, recv_sem=rs,
                                            device_id={'expert': to}, device_id_type=MESH)

    def w_copies(e, f):
        if f < nf:
            return [pltpu.make_async_copy(w.at[e, :, pl.ds(f * FC, FC)], wbuf.at[f, :, pl.ds(s * FC, FC)], wsem.at[f, s])
                    for s, w in enumerate((w1_hbm, w3_hbm))]
        return [pltpu.make_async_copy(w.at[e, :, pl.ds(nf * FC, tail)], wtail.at[:, pl.ds(s * tail, tail)], wsem.at[nf, s])
                for s, w in enumerate((w1_hbm, w3_hbm))]

    def w2_ref(odd, e):
        return xall.at[pl.ds(0, ff), pl.ds(e * DC, DC)] if odd else w2buf.at[e]

    def w2_copy(q, odd, e):
        cols = pl.ds(pl.multiple_of(q * DC, DC), DC)
        return pltpu.make_async_copy(w2_hbm.at[e, :, cols], w2_ref(odd, e), w2sem.at[odd, e])

    def piece(b, p, ss, to):
        r = pl.ds(pl.multiple_of(b * t + p * pt, pt), pt)
        return remote(xall.at[r], xall.at[r], ss, xrecv.at[b, p], to)

    def meta(b, ss, to):
        return remote(mall.at[b], mall.at[b], ss, mrecv.at[b], to)

    def got(b, p):
        piece(b, p, xsend_s.at[0, p], sib).wait_recv()

    def got_meta(b):
        meta(b, msend.at[0], sib).wait_recv()

    def to_sib(o, p):
        return piece(dev(o, k), p, xsend_s.at[o, p], sib)

    def own_right(p):
        return piece(me, p, xsend_r.at[p], right)

    def own_left(p):
        return piece(me, p, xsend_l.at[p], left)

    def relay_right(p):
        return piece(left, p, xsend_r.at[PIECES + p], right)

    def relay_left(p):
        return piece(right, hp + p, xsend_l.at[PIECES + p], left)

    def token_sends():
        out = [to_sib(o, p) for o in range(CHIPS) for p in range(PIECES)]
        out += [own_right(p) for p in range(PIECES)] + [own_left(p) for p in range(PIECES)]
        return out + [relay_right(p) for p in range(hp)] + [relay_left(p) for p in range(hp)]

    def send_own():
        for p in range(PIECES):
            own_right(p).start()
            own_left((p + hp) % PIECES).start()
        for p in range(PIECES):
            to_sib(0, p).start()

    def relay(p):
        got(left, p)
        relay_right(p).start()
        got(right, hp + p)
        relay_left(p).start()

    def sib_near(first):
        for p in range(hp):
            q = p if first else hp + p
            to_sib(3, q).start()
            to_sib(1, hp + p if first else p).start()

    def rest_near():
        for p in range(hp):
            got(left, hp + p)
            got(right, p)

    def far_in():
        for p in range(hp):
            got(far, p)
            to_sib(2, p).start()
            got(far, hp + p)
            to_sib(2, hp + p).start()

    def wait_block(b):
        for p in range(PIECES):
            got(b, p)

    def spot(o):
        return {0: 0, 3: 1, 1: 2, 2: 3}[o]

    def gather(beta, o):
        b = dev(o, beta)
        ids = mall[b, 0:8]
        gts = mall[b, 8:16]
        for e in range(el):
            eq = ids == (me * el + e).astype(F32)
            pos[0, o, e:e + 1, :] = jnp.sum(eq.astype(F32), axis=0, keepdims=True)
            pos[1, o, e:e + 1, :] = jnp.sum(jnp.where(eq, gts, 0.0), axis=0, keepdims=True)
        m = pos[0, o]
        before = _dot(m.astype(BF16), tri[...])
        rank = jnp.where(m > 0.0, before, -1.0)
        pos[0, o] = rank
        row = _iota((cap, t), 0).astype(F32)
        for e in range(el):
            pmat[e] = (rank[e:e + 1, :] == row).astype(BF16)
        hrow = _iota((extra, t), 0).astype(F32) + float(cap)
        phot[...] = jnp.logical_and(rank[0:1, :] == hrow, me == 0).astype(BF16)
        block = pl.ds(pl.multiple_of(b * t, t), t)

        def cols(j, _):
            w = pl.ds(pl.multiple_of(j * 512, 512), 512)
            xb = xall[block, w]
            r = _dot(pmat[...].reshape(el * cap, t), xb).astype(BF16).reshape(el, cap, 512)
            for e in range(el):
                xg[e, o, :, w] = r[e]
            xhot[spot(o), :, w] = _dot(phot[...], xb).astype(BF16)
            return 0

        lax.fori_loop(0, d // 512, cols, 0, unroll=True)

    def act(r, w, width):
        ab = _dot(r, w)
        a, b = ab[:, :width], ab[:, width:]
        return (a * jax.nn.sigmoid(a) * b).astype(BF16)

    def up_hot(blocks, f, w_ref, width):
        lo, hi = blocks
        uhot[lo * extra:hi * extra, f * FC:f * FC + width] = act(xhot[lo:hi].reshape((hi - lo) * extra, d), w_ref[...], width)

    def w_slot(f):
        return (wbuf.at[f], FC) if f < nf else (wtail, tail)

    def up_hot_near():
        for f in range(nf + 1):
            for cp in w_copies(0, f):
                cp.wait()

        @pl.when(me == 0)
        def _():
            for f in range(nf + 1):
                up_hot((0, CHIPS - 1), f, *w_slot(f))

    def up(beta, hook):
        def body(i, _):
            e = i if beta == 0 else el - 1 - i
            after = jnp.minimum(e + 1, el - 1) if beta == 0 else jnp.maximum(e - 1, 0)
            hook(i)
            lhs = xg[e].reshape(rows, d)

            for f in range(nf + 1):
                @pl.when(i > 0)
                def _():
                    for cp in w_copies(e, f):
                        cp.wait()
                w_ref, width = w_slot(f)
                w_cols = pl.ds(f * FC, width)
                u[e, :, w_cols] = act(lhs, w_ref[...], width)

                @pl.when(jnp.logical_and(me == 0, e == 0))
                def _():
                    up_hot((CHIPS - 1 if beta == 0 else 0, CHIPS), f, w_ref, width)

                @pl.when(i + 1 < el)
                def _():
                    for cp in w_copies(after, f):
                        cp.start()
            return 0

        lax.fori_loop(0, el, body, 0)

    def d_copy(q):
        return remote(psib.at[q % 2], drecv.at[q % 2], dsend.at[q % 2], drs.at[q % 2], sib)

    def f_copies(q):
        return [remote(pown.at[q, 2, s], frecv.at[q, s], fsend.at[q, s], frs.at[q, s], to)
                for s, to in enumerate((right, left))]

    def n_copies(q):
        return [remote(pown.at[q, o], nrecv.at[q, s], nsend.at[q, s], nrs.at[q, s], to)
                for s, (o, to) in enumerate(((1, right), (3, left)))]

    def pair_add(q):
        d_copy(q).wait_recv()
        for o in (2, 1, 3, 0):
            pown[q, o] = psib[q % 2, o] + drecv[q % 2, o]
        for cp in f_copies(q):
            cp.start()

        @pl.when(q < nq - 2)
        def _():
            pl.semaphore_signal(credit, inc=1, device_id={'expert': sib}, device_id_type=MESH)

    def relay_add(q):
        for cp in f_copies(q):
            cp.wait_recv()
        pown[q, 1, 0] = pown[q, 1, 0] + frecv[q, 0]
        pown[q, 3, 1] = pown[q, 3, 1] + frecv[q, 1]
        for cp in n_copies(q):
            cp.start()

    def finish(q, _):
        for cp in n_copies(q):
            cp.wait_recv()
        for s in range(2):
            y = pown[q, 0, s] + nrecv[q, 0, s] + nrecv[q, 1, s]
            out_ref[:, pl.ds(pl.multiple_of(q * DC + s * half, half), half)] = y.astype(BF16)
        return 0

    def build_scatter():
        cat[...] = jnp.zeros_like(cat)
        for o in range(CHIPS):
            cat[o * el:(o + 1) * el, :] = pos[0, o]
            cat[(CHIPS + o) * el:(CHIPS + o + 1) * el, :] = pos[1, o]
        cols = jnp.transpose(cat[...])
        g1 = cols.astype(BF16)
        r1 = cols - g1.astype(F32)
        g2 = r1.astype(BF16)
        g3 = (r1 - g2.astype(F32)).astype(BF16)
        lane = _iota((1, wide), 1)
        slot_e = jnp.zeros((1, wide), jnp.int32)
        for e in range(1, el):
            slot_e = slot_e + (lane >= e * cap).astype(jnp.int32)
        want = (lane - cap * slot_e).astype(F32)
        depth = cat.shape[0]

        def build(o, _):
            rr = _iota((depth, wide), 0)
            ll = _iota((depth, wide), 1)

            def pick(first):
                lo = (rr - first) * cap
                cold = jnp.logical_and(jnp.logical_and(ll >= lo, ll < lo + cap), ll < el * cap)
                more = jnp.logical_and(jnp.logical_and(rr == first, ll >= el * cap), me == 0)
                return jnp.logical_or(cold, more).astype(BF16)

            gate = pick((CHIPS + o) * el)
            hit = _dot(g1, pick(o * el)) == want
            for s, gs in enumerate((g1, g2, g3)):
                s_all[o, s] = jnp.where(hit, _dot(gs, gate), 0.0).astype(BF16)
            return 0

        lax.fori_loop(0, CHIPS, build, 0)

    def chunk(beta, q, odd):
        def next_w2():
            nxt = (q + 1) % nq
            for e in range(el):
                w2_copy(nxt, 1 - odd, e).start()

        if beta == 0 or not odd:
            next_w2()
        else:
            pl.when(q + 1 < nq)(next_w2)
        for e0 in range(0, el, 8):
            for e in range(e0, e0 + 8):
                w2_copy(q, odd, e).wait()
            for e in range(e0, e0 + 8):
                h = _dot(u[e], w2_ref(odd, e)[...]).astype(BF16).reshape(CHIPS, cap, DC)
                for o in range(CHIPS):
                    hbuf[o, e * cap:(e + 1) * cap] = h[o]

        @pl.when(me == 0)
        def _():
            h = _dot(uhot[...], w2_ref(odd, 0)[...]).astype(BF16).reshape(CHIPS, extra, DC)
            for o in range(CHIPS):
                hbuf[o, el * cap:] = h[spot(o)]

        @pl.when(jnp.logical_and(k != beta, q >= 2))
        def _():
            d_copy(q - 2).wait_send()

        for o in range(CHIPS):
            hb = hbuf[o]
            r = _dot(s_all[o, 0], hb) + _dot(s_all[o, 1], hb) + _dot(s_all[o, 2], hb)
            psib[q % 2, o, 0] = r[:, :half]
            psib[q % 2, o, 1] = r[:, half:]

        @pl.when(k != beta)
        def _():
            @pl.when(q >= 2)
            def _():
                pl.semaphore_wait(credit, 1)
            d_copy(q).start()

    def down_phase(beta):
        def step(j, _):
            for odd in range(2):
                i = 2 * j + odd

                @pl.when(jnp.logical_and(k == beta, i >= 1))
                def _():
                    pair_add(i - 1)

                if beta == 0 and odd:
                    @pl.when(jnp.logical_and(k == beta, i >= 3))
                    def _():
                        relay_add(j - 1)
                if beta == 1:
                    @pl.when(jnp.logical_and(k == beta, i >= 3))
                    def _():
                        relay_add(i - 3)

                chunk(beta, i, odd)
            return 0

        lax.fori_loop(0, nq // 2, step, 0)

        @pl.when(k == beta)
        def _():
            pair_add(nq - 1)
            if beta == 1:
                for q in range(nq - 3, nq):
                    relay_add(q)

        @pl.when(k != beta)
        def _():
            for q in range(nq - 2, nq):
                d_copy(q).wait_send()

    own = pltpu.make_async_copy(x_hbm, xall.at[pl.ds(pl.multiple_of(me * t, t), t)], loc_sem.at[0])
    own_i = pltpu.make_async_copy(idx_hbm, idx_v, loc_sem.at[1])
    own_g = pltpu.make_async_copy(g_hbm, g_v, loc_sem.at[2])
    own.start()
    own_i.start()
    own_g.start()
    turn[...] = jnp.full(turn.shape, -1.0, F32)
    barrier = pltpu.get_barrier_semaphore()
    for peer in (sib, right, left):
        pl.semaphore_signal(barrier, inc=1, device_id={'expert': peer}, device_id_type=MESH)
    pl.semaphore_wait(barrier, 3)
    own.wait()

    @pl.when(k == 0)
    def _():
        send_own()

    own_i.wait()
    own_g.wait()
    turn[:, 0:top] = idx_v[...].astype(F32)
    turn[:, 8:8 + top] = g_v[...]
    mall[me] = jnp.transpose(turn[...])[0:16]
    metas = [meta(me, msend.at[0], sib), meta(me, msend.at[1], right), meta(me, msend.at[2], left)]
    for cp in metas:
        cp.start()
    for f in range(nf + 1):
        for cp in w_copies(0, f):
            cp.start()
    for e in range(el):
        w2_copy(0, 0, e).start()
    hbuf[:, el * cap:, :] = jnp.zeros((CHIPS, extra, DC), BF16)
    tri[...] = (_iota((t, t), 0) < _iota((t, t), 1)).astype(BF16)

    got_meta(left)
    metas += [meta(left, msend.at[3], right), meta(left, msend.at[4], sib)]
    metas[3].start()
    metas[4].start()
    got_meta(right)
    metas += [meta(right, msend.at[5], sib)]
    metas[5].start()
    got_meta(far)
    metas += [meta(far, msend.at[6], sib)]
    metas[6].start()
    for o in range(CHIPS):
        got_meta(dev(o, 1 - k))

    @pl.when(k == 1)
    def _():
        wait_block(dev(0, 0))

    gather(0, 0)

    @pl.when(k == 0)
    def _():
        for p in range(hp):
            relay(p)
        sib_near(True)
        rest_near()
        sib_near(False)

    @pl.when(k == 1)
    def _():
        wait_block(dev(3, 0))
        wait_block(dev(1, 0))

    gather(0, 3)
    gather(0, 1)
    up_hot_near()

    @pl.when(k == 0)
    def _():
        far_in()

    @pl.when(k == 1)
    def _():
        wait_block(dev(2, 0))
        send_own()

    gather(0, 2)

    def hook_first(i):
        pl.when(i == 5)(build_scatter)

        @pl.when(k == 1)
        def _():
            for at, p in ((1, 0), (2, 1)):
                @pl.when(i == at)
                def _():
                    relay(p)

            @pl.when(i == 4)
            def _():
                rest_near()
                sib_near(True)
                sib_near(False)

            @pl.when(i == 6)
            def _():
                far_in()

    up(0, hook_first)

    @pl.when(k == 0)
    def _():
        for o in range(CHIPS):
            wait_block(dev(o, 1))

    for o in range(CHIPS):
        gather(1, o)
    for cp in token_sends():
        cp.wait_send()
    down_phase(0)

    def hook_second(i):
        pl.when(i == 5)(build_scatter)

        @pl.when(jnp.logical_and(k == 0, i < nq - 3))
        def _():
            relay_add(3 + i)

    up(1, hook_second)
    down_phase(1)
    lax.fori_loop(0, nq, finish, 0)

    for cp in metas:
        cp.wait_send()
    for q in range(nq):
        for cp in f_copies(q) + n_copies(q):
            cp.wait_send()


def solution(mesh):
    n = mesh.shape['expert']
    assert n == 2 * CHIPS

    def local(x, idx, g, hot_tok, w1, w3, w2):
        t, d = x.shape
        k = idx.shape[1]
        el, _, ff = w1.shape
        e = el * n
        hot = hot_tok.shape[0]
        most = 2 * ((t * k - hot + e - 2) // (e - 1))
        cap = -(-most // 16) * 16
        extra = hot - cap
        half = DC // 2
        nf, nq = ff // FC, d // DC
        tail = ff - nf * FC
        assert k <= 8
        dma, any_ = pltpu.SemaphoreType.DMA, pl.BlockSpec(memory_space=pl.ANY)
        vm = pltpu.VMEM
        return pl.pallas_call(
            functools.partial(_kernel, cap, hot),
            out_shape=jax.ShapeDtypeStruct((t, d), BF16),
            in_specs=[any_] * 6,
            out_specs=pl.BlockSpec(memory_space=pltpu.VMEM),
            scratch_shapes=[
                vm((n * t, d), BF16), vm((n, 16, t), F32), vm((2, CHIPS, el, t), F32),
                vm((el, CHIPS, cap, d), BF16), vm((CHIPS, extra, d), BF16),
                vm((el, CHIPS * cap, ff), BF16), vm((CHIPS * extra, ff), BF16),
                vm((nf, d, 2 * FC), BF16), vm((d, 2 * tail), BF16), vm((el, ff, DC), BF16),
                vm((CHIPS, 3, t, el * cap + extra), BF16),
                vm((CHIPS, el * cap + extra, DC), BF16),
                vm((nq, CHIPS, 2, t, half), F32), vm((2, CHIPS, 2, t, half), F32), vm((2, CHIPS, 2, t, half), F32),
                vm((nq, 2, t, half), F32), vm((nq, 2, 2, t, half), F32),
                vm((-(-2 * CHIPS * el // 128) * 128, t), F32), vm((el, cap, t), BF16), vm((extra, t), BF16), vm((t, t), BF16),
                vm((t, k), jnp.int32), vm((t, k), F32), vm((t, 128), F32),
                dma((3,)), dma((CHIPS, PIECES)), dma((2 * PIECES,)), dma((2 * PIECES,)), dma((n, PIECES)), dma((7,)), dma((n,)),
                dma((nf + 1, 2)), dma((2, el)), dma((2,)), dma((2,)), dma((nq, 2)), dma((nq, 2)), dma((nq, 2)), dma((nq, 2)),
                pltpu.SemaphoreType.REGULAR,
            ],
            compiler_params=pltpu.CompilerParams(collective_id=0, has_side_effects=True, vmem_limit_bytes=67043328),
        )(x, idx, g, w1, w3, w2)

    rows = P(('data', 'expert'))
    wspec = P('expert')
    return jax.shard_map(local, mesh=mesh, in_specs=(rows, rows, rows, rows, wspec, wspec, wspec), out_specs=rows, check_vma=False)
```

```python
import functools

import jax
import jax.numpy as jnp
from jax import lax
from jax.experimental import pallas as pl
from jax.experimental.pallas import tpu as pltpu
from jax.sharding import PartitionSpec as P

MESH = pl.DeviceIdType.MESH
F32 = jnp.float32
BF16 = jnp.bfloat16
CHIPS = 4
PIECES = 4
FC = 256
DC = 256


def _dot(a, b):
    return jnp.dot(a, b, preferred_element_type=F32)


def _iota(shape, dim):
    return lax.broadcasted_iota(jnp.int32, shape, dim)


def _kernel(cap, hot, x_hbm, idx_hbm, g_hbm, w1_hbm, w3_hbm, w2_hbm, out_ref,
            xall, mall, pos, xg, xhot, u, uhot, wbuf, wtail, w2buf, s_all, hbuf,
            pown, psib, drecv, frecv, nrecv, cat, pmat, phot, tri, idx_v, g_v, routes,
            loc_sem, xsend_s, xsend_r, xsend_l, xrecv, msend, mrecv,
            wsem, w2sem, dsend, drs, fsend, frs, nsend, nrs, credit):
    me = lax.axis_index('expert')
    c, k = me // 2, me % 2

    def dev(o, kk):
        return ((c + o) % CHIPS) * 2 + kk

    sib, right, left, far = dev(0, 1 - k), dev(1, k), dev(3, k), dev(2, k)
    t, d = x_hbm.shape
    top = idx_hbm.shape[0]
    el, _, ff = w1_hbm.shape
    nf = ff // FC
    tail = ff - nf * FC
    extra = hot - cap
    nq = d // DC
    half = DC // 2
    pt = t // PIECES
    hp = PIECES // 2
    rows = CHIPS * cap
    wide = el * cap + extra

    def remote(src, dst, ss, rs, to):
        return pltpu.make_async_remote_copy(src_ref=src, dst_ref=dst, send_sem=ss, recv_sem=rs,
                                            device_id={'expert': to}, device_id_type=MESH)

    def w_copies(e, f):
        if f < nf:
            return [pltpu.make_async_copy(w.at[e, :, pl.ds(f * FC, FC)], wbuf.at[f, :, pl.ds(s * FC, FC)], wsem.at[f, s])
                    for s, w in enumerate((w1_hbm, w3_hbm))]
        return [pltpu.make_async_copy(w.at[e, :, pl.ds(nf * FC, tail)], wtail.at[:, pl.ds(s * tail, tail)], wsem.at[nf, s])
                for s, w in enumerate((w1_hbm, w3_hbm))]

    def w2_ref(odd, e):
        return xall.at[pl.ds(0, ff), pl.ds(e * DC, DC)] if odd else w2buf.at[e]

    def w2_copy(q, odd, e):
        cols = pl.ds(pl.multiple_of(q * DC, DC), DC)
        return pltpu.make_async_copy(w2_hbm.at[e, :, cols], w2_ref(odd, e), w2sem.at[odd, e])

    def piece(b, p, ss, to):
        r = pl.ds(pl.multiple_of(b * t + p * pt, pt), pt)
        return remote(xall.at[r], xall.at[r], ss, xrecv.at[b, p], to)

    def meta(b, ss, to):
        return remote(mall.at[b], mall.at[b], ss, mrecv.at[b], to)

    def got(b, p):
        piece(b, p, xsend_s.at[0, p], sib).wait_recv()

    def got_meta(b):
        meta(b, msend.at[0], sib).wait_recv()

    def to_sib(o, p):
        return piece(dev(o, k), p, xsend_s.at[o, p], sib)

    def own_right(p):
        return piece(me, p, xsend_r.at[p], right)

    def own_left(p):
        return piece(me, p, xsend_l.at[p], left)

    def relay_right(p):
        return piece(left, p, xsend_r.at[PIECES + p], right)

    def relay_left(p):
        return piece(right, hp + p, xsend_l.at[PIECES + p], left)

    def token_sends():
        out = [to_sib(o, p) for o in range(CHIPS) for p in range(PIECES)]
        out += [own_right(p) for p in range(PIECES)] + [own_left(p) for p in range(PIECES)]
        return out + [relay_right(p) for p in range(hp)] + [relay_left(p) for p in range(hp)]

    def send_own():
        for p in range(PIECES):
            own_right(p).start()
            own_left((p + hp) % PIECES).start()
        for p in range(PIECES):
            to_sib(0, p).start()

    def relay(p):
        got(left, p)
        relay_right(p).start()
        got(right, hp + p)
        relay_left(p).start()

    def sib_near(first):
        for p in range(hp):
            q = p if first else hp + p
            to_sib(3, q).start()
            to_sib(1, hp + p if first else p).start()

    def rest_near():
        for p in range(hp):
            got(left, hp + p)
            got(right, p)

    def far_in():
        for p in range(hp):
            got(far, p)
            to_sib(2, p).start()
            got(far, hp + p)
            to_sib(2, hp + p).start()

    def wait_block(b):
        for p in range(PIECES):
            got(b, p)

    def spot(o):
        return {0: 0, 3: 1, 1: 2, 2: 3}[o]

    def gather(beta, o):
        b = dev(o, 1 - beta)
        pl.when(b != me)(lambda: got_meta(b))
        ids = mall[b, 0:8]
        gts = mall[b, 8:16]
        for e in range(el):
            eq = ids == (me * el + e).astype(F32)
            pos[0, o, e:e + 1, :] = jnp.sum(eq.astype(F32), axis=0, keepdims=True)
            pos[1, o, e:e + 1, :] = jnp.sum(jnp.where(eq, gts, 0.0), axis=0, keepdims=True)
        m = pos[0, o]
        before = _dot(m.astype(BF16), tri[...])
        rank = jnp.where(m > 0.0, before, -1.0)
        pos[0, o] = rank
        row = _iota((cap, t), 0).astype(F32)
        for e in range(el):
            pmat[e] = (rank[e:e + 1, :] == row).astype(BF16)
        hrow = _iota((extra, t), 0).astype(F32) + float(cap)
        phot[...] = jnp.logical_and(rank[0:1, :] == hrow, me == 0).astype(BF16)
        block = pl.ds(pl.multiple_of(b * t, t), t)

        def cols(j, _):
            w = pl.ds(pl.multiple_of(j * 512, 512), 512)
            xb = xall[block, w]
            r = _dot(pmat[...].reshape(el * cap, t), xb).astype(BF16).reshape(el, cap, 512)
            for e in range(el):
                xg[e, o, :, w] = r[e]
            xhot[spot(o), :, w] = _dot(phot[...], xb).astype(BF16)
            return 0

        lax.fori_loop(0, d // 512, cols, 0, unroll=True)

    def act(r, w, width):
        ab = _dot(r, w)
        a, b = ab[:, :width], ab[:, width:]
        return (a * jax.nn.sigmoid(a) * b).astype(BF16)

    def up_hot(blocks, f, w_ref, width):
        lo, hi = blocks
        uhot[lo * extra:hi * extra, f * FC:f * FC + width] = act(xhot[lo:hi].reshape((hi - lo) * extra, d), w_ref[...], width)

    def w_slot(f):
        return (wbuf.at[f], FC) if f < nf else (wtail, tail)

    def up_hot_near():
        for f in range(nf + 1):
            for cp in w_copies(0, f):
                cp.wait()

        @pl.when(me == 0)
        def _():
            for f in range(nf + 1):
                up_hot((0, CHIPS - 1), f, *w_slot(f))

    def up(beta, hook):
        def body(i, _):
            e = i if beta == 0 else el - 1 - i
            after = jnp.minimum(e + 1, el - 1) if beta == 0 else jnp.maximum(e - 1, 0)
            hook(i)
            lhs = xg[e].reshape(rows, d)

            for f in range(nf + 1):
                @pl.when(i > 0)
                def _():
                    for cp in w_copies(e, f):
                        cp.wait()
                w_ref, width = w_slot(f)
                w_cols = pl.ds(f * FC, width)
                u[e, :, w_cols] = act(lhs, w_ref[...], width)

                @pl.when(jnp.logical_and(me == 0, e == 0))
                def _():
                    up_hot((CHIPS - 1 if beta == 0 else 0, CHIPS), f, w_ref, width)

                @pl.when(i + 1 < el)
                def _():
                    for cp in w_copies(after, f):
                        cp.start()
            return 0

        lax.fori_loop(0, el, body, 0)

    def d_copy(q):
        return remote(psib.at[q % 2], drecv.at[q % 2], dsend.at[q % 2], drs.at[q % 2], sib)

    def f_copies(q):
        return [remote(pown.at[q, 2, s], frecv.at[q, s], fsend.at[q, s], frs.at[q, s], to)
                for s, to in enumerate((right, left))]

    def n_copies(q):
        return [remote(pown.at[q, o], nrecv.at[q, s], nsend.at[q, s], nrs.at[q, s], to)
                for s, (o, to) in enumerate(((1, right), (3, left)))]

    def pair_add(q):
        d_copy(q).wait_recv()
        for o in (2, 1, 3, 0):
            pown[q, o] = psib[q % 2, o] + drecv[q % 2, o]
        for cp in f_copies(q):
            cp.start()

        @pl.when(q < nq - 2)
        def _():
            pl.semaphore_signal(credit, inc=1, device_id={'expert': sib}, device_id_type=MESH)

    def relay_add(q):
        for cp in f_copies(q):
            cp.wait_recv()
        pown[q, 1, 0] = pown[q, 1, 0] + frecv[q, 0]
        pown[q, 3, 1] = pown[q, 3, 1] + frecv[q, 1]
        for cp in n_copies(q):
            cp.start()

    def finish(q, _):
        for cp in n_copies(q):
            cp.wait_recv()
        for s in range(2):
            y = pown[q, 0, s] + nrecv[q, 0, s] + nrecv[q, 1, s]
            out_ref[:, pl.ds(pl.multiple_of(q * DC + s * half, half), half)] = y.astype(BF16)
        return 0

    def build_scatter():
        cat[...] = jnp.zeros_like(cat)
        for o in range(CHIPS):
            cat[o * el:(o + 1) * el, :] = pos[0, o]
            cat[(CHIPS + o) * el:(CHIPS + o + 1) * el, :] = pos[1, o]
        cols = jnp.transpose(cat[...])
        g1 = cols.astype(BF16)
        r1 = cols - g1.astype(F32)
        g2 = r1.astype(BF16)
        g3 = (r1 - g2.astype(F32)).astype(BF16)
        lane = _iota((1, wide), 1)
        slot_e = jnp.zeros((1, wide), jnp.int32)
        for e in range(1, el):
            slot_e = slot_e + (lane >= e * cap).astype(jnp.int32)
        want = (lane - cap * slot_e).astype(F32)
        depth = cat.shape[0]

        def build(o, _):
            rr = _iota((depth, wide), 0)
            ll = _iota((depth, wide), 1)

            def pick(first):
                lo = (rr - first) * cap
                cold = jnp.logical_and(jnp.logical_and(ll >= lo, ll < lo + cap), ll < el * cap)
                more = jnp.logical_and(jnp.logical_and(rr == first, ll >= el * cap), me == 0)
                return jnp.logical_or(cold, more).astype(BF16)

            gate = pick((CHIPS + o) * el)
            hit = _dot(g1, pick(o * el)) == want
            for s, gs in enumerate((g1, g2, g3)):
                s_all[o, s] = jnp.where(hit, _dot(gs, gate), 0.0).astype(BF16)
            return 0

        lax.fori_loop(0, CHIPS, build, 0)

    def chunk(beta, q, odd):
        def next_w2():
            nxt = (q + 1) % nq
            for e in range(el):
                w2_copy(nxt, 1 - odd, e).start()

        if beta == 0 or not odd:
            next_w2()
        else:
            pl.when(q + 1 < nq)(next_w2)
        for e0 in range(0, el, 8):
            for e in range(e0, e0 + 8):
                w2_copy(q, odd, e).wait()
            for e in range(e0, e0 + 8):
                h = _dot(u[e], w2_ref(odd, e)[...]).astype(BF16).reshape(CHIPS, cap, DC)
                for o in range(CHIPS):
                    hbuf[o, e * cap:(e + 1) * cap] = h[o]

        @pl.when(me == 0)
        def _():
            h = _dot(uhot[...], w2_ref(odd, 0)[...]).astype(BF16).reshape(CHIPS, extra, DC)
            for o in range(CHIPS):
                hbuf[o, el * cap:] = h[spot(o)]

        @pl.when(jnp.logical_and(k == beta, q >= 2))
        def _():
            d_copy(q - 2).wait_send()

        for o in range(CHIPS):
            hb = hbuf[o]
            r = _dot(s_all[o, 0], hb) + _dot(s_all[o, 1], hb) + _dot(s_all[o, 2], hb)
            psib[q % 2, o, 0] = r[:, :half]
            psib[q % 2, o, 1] = r[:, half:]

        @pl.when(k == beta)
        def _():
            @pl.when(q >= 2)
            def _():
                pl.semaphore_wait(credit, 1)
            d_copy(q).start()

    def down_phase(beta):
        def step(j, _):
            for odd in range(2):
                i = 2 * j + odd

                @pl.when(jnp.logical_and(k != beta, i >= 1))
                def _():
                    pair_add(i - 1)

                if beta == 0 and odd:
                    @pl.when(jnp.logical_and(k != beta, i >= 3))
                    def _():
                        relay_add(j - 1)
                if beta == 1:
                    @pl.when(jnp.logical_and(k != beta, i >= 3))
                    def _():
                        relay_add(i - 3)

                chunk(beta, i, odd)
            return 0

        lax.fori_loop(0, nq // 2, step, 0)

        @pl.when(k != beta)
        def _():
            pair_add(nq - 1)
            if beta == 1:
                for q in range(nq - 3, nq):
                    relay_add(q)

        @pl.when(k == beta)
        def _():
            for q in range(nq - 2, nq):
                d_copy(q).wait_send()

    own = pltpu.make_async_copy(x_hbm, xall.at[pl.ds(pl.multiple_of(me * t, t), t)], loc_sem.at[0])
    own_i = pltpu.make_async_copy(idx_hbm, idx_v, loc_sem.at[1])
    own_g = pltpu.make_async_copy(g_hbm, g_v, loc_sem.at[2])
    own.start()
    own_i.start()
    own_g.start()
    barrier = pltpu.get_barrier_semaphore()
    peers = [far, right, left, sib] + [dev(o, 1 - k) for o in (2, 1, 3)]
    for peer in peers:
        pl.semaphore_signal(barrier, inc=1, device_id={'expert': peer}, device_id_type=MESH)
    pl.semaphore_wait(barrier, len(peers))
    own.wait()
    own_i.wait()
    own_g.wait()
    routes[...] = jnp.full(routes.shape, -1.0, F32)
    routes[0:top] = idx_v[...].astype(F32)
    routes[8:8 + top] = g_v[...]
    mall[me] = routes[...]
    metas = [meta(me, msend.at[j], to) for j, to in enumerate(peers)]
    for cp in metas:
        cp.start()

    @pl.when(k == 1)
    def _():
        send_own()

    for f in range(nf + 1):
        for cp in w_copies(0, f):
            cp.start()
    for e in range(el):
        w2_copy(0, 0, e).start()
    hbuf[:, el * cap:, :] = jnp.zeros((CHIPS, extra, DC), BF16)
    tri[...] = (_iota((t, t), 0) < _iota((t, t), 1)).astype(BF16)

    @pl.when(k == 0)
    def _():
        wait_block(dev(0, 1))

    gather(0, 0)

    @pl.when(k == 1)
    def _():
        for p in range(hp):
            relay(p)
        sib_near(True)
        rest_near()
        sib_near(False)

    @pl.when(k == 0)
    def _():
        wait_block(dev(3, 1))
        wait_block(dev(1, 1))

    gather(0, 3)
    gather(0, 1)
    up_hot_near()

    @pl.when(k == 1)
    def _():
        far_in()

    @pl.when(k == 0)
    def _():
        wait_block(dev(2, 1))
        send_own()

    gather(0, 2)

    def hook_first(i):
        pl.when(i == 5)(build_scatter)

        @pl.when(k == 0)
        def _():
            for at, p in ((1, 0), (2, 1)):
                @pl.when(i == at)
                def _():
                    relay(p)

            @pl.when(i == 4)
            def _():
                rest_near()
                sib_near(True)
                sib_near(False)

            @pl.when(i == 6)
            def _():
                far_in()

    up(0, hook_first)

    @pl.when(k == 1)
    def _():
        for o in range(CHIPS):
            wait_block(dev(o, 0))

    for o in range(CHIPS):
        gather(1, o)
    for cp in token_sends():
        cp.wait_send()
    down_phase(0)

    def hook_second(i):
        pl.when(i == 5)(build_scatter)

        @pl.when(jnp.logical_and(k == 1, i < nq - 3))
        def _():
            relay_add(3 + i)

    up(1, hook_second)
    down_phase(1)
    lax.fori_loop(0, nq, finish, 0)

    for cp in metas:
        cp.wait_send()
    for q in range(nq):
        for cp in f_copies(q) + n_copies(q):
            cp.wait_send()


def solution(mesh):
    n = mesh.shape['expert']
    assert n == 2 * CHIPS

    def local(x, idx, g, hot_tok, w1, w3, w2):
        t, d = x.shape
        k = idx.shape[1]
        el, _, ff = w1.shape
        e = el * n
        hot = hot_tok.shape[0]
        most = 2 * ((t * k - hot + e - 2) // (e - 1))
        cap = -(-most // 16) * 16
        extra = hot - cap
        half = DC // 2
        nf, nq = ff // FC, d // DC
        tail = ff - nf * FC
        assert k <= 8
        dma, any_ = pltpu.SemaphoreType.DMA, pl.BlockSpec(memory_space=pl.ANY)
        vm = pltpu.VMEM
        return pl.pallas_call(
            functools.partial(_kernel, cap, hot),
            out_shape=jax.ShapeDtypeStruct((t, d), BF16),
            in_specs=[any_] * 6,
            out_specs=pl.BlockSpec(memory_space=pltpu.VMEM),
            scratch_shapes=[
                vm((n * t, d), BF16), vm((n, 16, t), F32), vm((2, CHIPS, el, t), F32),
                vm((el, CHIPS, cap, d), BF16), vm((CHIPS, extra, d), BF16),
                vm((el, CHIPS * cap, ff), BF16), vm((CHIPS * extra, ff), BF16),
                vm((nf, d, 2 * FC), BF16), vm((d, 2 * tail), BF16), vm((el, ff, DC), BF16),
                vm((CHIPS, 3, t, el * cap + extra), BF16),
                vm((CHIPS, el * cap + extra, DC), BF16),
                vm((nq, CHIPS, 2, t, half), F32), vm((2, CHIPS, 2, t, half), F32), vm((2, CHIPS, 2, t, half), F32),
                vm((nq, 2, t, half), F32), vm((nq, 2, 2, t, half), F32),
                vm((-(-2 * CHIPS * el // 128) * 128, t), F32), vm((el, cap, t), BF16), vm((extra, t), BF16), vm((t, t), BF16),
                vm((k, t), jnp.int32), vm((k, t), F32), vm((16, t), F32),
                dma((3,)), dma((CHIPS, PIECES)), dma((2 * PIECES,)), dma((2 * PIECES,)), dma((n, PIECES)), dma((7,)), dma((n,)),
                dma((nf + 1, 2)), dma((2, el)), dma((2,)), dma((2,)), dma((nq, 2)), dma((nq, 2)), dma((nq, 2)), dma((nq, 2)),
                pltpu.SemaphoreType.REGULAR,
            ],
            compiler_params=pltpu.CompilerParams(collective_id=0, has_side_effects=True, vmem_limit_bytes=67043328),
        )(x, idx.T, g.T, w1, w3, w2)

    rows = P(('data', 'expert'))
    wspec = P('expert')
    return jax.shard_map(local, mesh=mesh, in_specs=(rows, rows, rows, rows, wspec, wspec, wspec), out_specs=rows, check_vma=False)
```
